16 devices in a mesh: data: 2 (over z), group: 8 (over y, x, core).
Axes of the slice: x: 2, y: 2, z: 2, core: 2. Of those that a mesh axis runs over, the one named last changes fastest.
Arguments:
- latents: bfloat16 [2048, 1152], P(('data', 'group')), parts along dimension 0
- hint_embed: bfloat16 [2048, 1152], P(('data', 'group')), parts along dimension 0
- in_qkv: bfloat16 [2, 13, 1152, 3456], replicated
- in_proj: bfloat16 [2, 13, 16, 72, 1152], replicated
- in_up: bfloat16 [2, 13, 1152, 4608], replicated
- in_down: bfloat16 [2, 13, 4608, 1152], replicated
- in_norm: bfloat16 [2, 13, 4, 1152], replicated
- out_qkv: bfloat16 [12, 1152, 3456], replicated
- out_proj: bfloat16 [12, 16, 72, 1152], replicated
- out_up: bfloat16 [12, 1152, 4608], replicated
- out_down: bfloat16 [12, 4608, 1152], replicated
- out_norm: bfloat16 [12, 4, 1152], replicated
- zero_proj: bfloat16 [13, 1152, 1152], replicated
- hint_proj: bfloat16 [1152, 1152], replicated
- skip_proj: bfloat16 [12, 2304, 1152], replicated
- final_norm: bfloat16 [2, 1152], replicated
- w_out: bfloat16 [1152, 1152], replicated
Outputs:
- output: bfloat16 [2048, 1152], P(('data', 'group')), parts along dimension 0
There are 2 independent parts. The reference program is written for one: setup_inputs(seed, part) draws one part's arguments, and reference() takes and returns one part's arrays. A program takes and returns all parts, laid end to end along the dimension named above; an argument that names none is the same for every part.
All inputs are finite; a program needn't handle non-finite values.
Results may differ from the reference program's by a relative error of at most 0.02.
Values are sent between devices in bfloat16 or wider.
A program may use at most 5 GiB of HBM per device.

```python
import math
import jax
import jax.numpy as jnp
from jax import lax

TOKENS = 1024
WIDTH = 1152
HEADS = 16
LAYERS = 12

HEAD_DIM = WIDTH // HEADS
IN_BLOCKS = LAYERS + 1
Q_GAIN = math.sqrt(max(1.0, math.log(TOKENS / 16.0)))
EPS = 1e-6


def draw_normal(rng_key, dim_sizes, std_scale):
    return (jax.random.normal(rng_key, dim_sizes, jnp.float32) * std_scale).astype(jnp.bfloat16)


def draw_qkv(rng_key, lead_dims):
    col_gain = jnp.concatenate([jnp.full((WIDTH,), Q_GAIN, jnp.float32), jnp.ones((2 * WIDTH,), jnp.float32)])
    raw_vals = jax.random.normal(rng_key, lead_dims + (WIDTH, 3 * WIDTH), jnp.float32)
    return (raw_vals * col_gain * WIDTH ** -0.5).astype(jnp.bfloat16)


def draw_norms(rng_key, lead_dims, row_count):
    centre = jnp.tile(jnp.array([1.0, 0.0], jnp.float32), row_count // 2)[:, None]
    raw_vals = jax.random.normal(rng_key, lead_dims + (row_count, WIDTH), jnp.float32)
    return (raw_vals * 0.2 + centre).astype(jnp.bfloat16)


def setup_inputs(seed: int = 0, part: int = 0) -> dict:
    part_keys = jax.random.split(jax.random.fold_in(jax.random.key(seed), part), 2)
    rng_keys = jax.random.split(jax.random.key(seed + 1), 15)
    in_lead = (2, IN_BLOCKS)
    out_lead = (LAYERS,)
    return {
        "latents": draw_normal(part_keys[0], (TOKENS, WIDTH), 1.0),
        "hint_embed": draw_normal(part_keys[1], (TOKENS, WIDTH), 1.0),
        "in_qkv": draw_qkv(rng_keys[0], in_lead),
        "in_proj": draw_normal(rng_keys[1], in_lead + (HEADS, HEAD_DIM, WIDTH), WIDTH ** -0.5),
        "in_up": draw_normal(rng_keys[2], in_lead + (WIDTH, 4 * WIDTH), WIDTH ** -0.5),
        "in_down": draw_normal(rng_keys[3], in_lead + (4 * WIDTH, WIDTH), (4 * WIDTH) ** -0.5),
        "in_norm": draw_norms(rng_keys[4], in_lead, 4),
        "out_qkv": draw_qkv(rng_keys[5], out_lead),
        "out_proj": draw_normal(rng_keys[6], out_lead + (HEADS, HEAD_DIM, WIDTH), WIDTH ** -0.5),
        "out_up": draw_normal(rng_keys[7], out_lead + (WIDTH, 4 * WIDTH), WIDTH ** -0.5),
        "out_down": draw_normal(rng_keys[8], out_lead + (4 * WIDTH, WIDTH), (4 * WIDTH) ** -0.5),
        "out_norm": draw_norms(rng_keys[9], out_lead, 4),
        "zero_proj": draw_normal(rng_keys[10], (IN_BLOCKS, WIDTH, WIDTH), 0.6 * WIDTH ** -0.5),
        "hint_proj": draw_normal(rng_keys[11], (WIDTH, WIDTH), WIDTH ** -0.5),
        "skip_proj": draw_normal(rng_keys[12], (LAYERS, 2 * WIDTH, WIDTH), (2 * WIDTH) ** -0.5),
        "final_norm": draw_norms(rng_keys[13], (), 2),
        "w_out": draw_normal(rng_keys[14], (WIDTH, WIDTH), WIDTH ** -0.5),
    }


def mat_f32(left_op, right_op):
    return jnp.dot(left_op, right_op, preferred_element_type=jnp.float32)


def layer_norm(values, norm_gain, norm_shift):
    wide_vals = values.astype(jnp.float32)
    centered = wide_vals - jnp.mean(wide_vals, axis=-1, keepdims=True)
    variance = jnp.mean(centered * centered, axis=-1, keepdims=True)
    normed = centered * lax.rsqrt(variance + EPS)
    return (normed * norm_gain.astype(jnp.float32) + norm_shift.astype(jnp.float32)).astype(jnp.bfloat16)


def head_attend(head_args):
    queries, key_rows, val_rows = head_args
    scores = mat_f32(queries, key_rows.T) * HEAD_DIM ** -0.5
    att_probs = jax.nn.softmax(scores, axis=-1).astype(jnp.bfloat16)
    return mat_f32(att_probs, val_rows).astype(jnp.bfloat16)


def transformer_block(residual, params):
    w_qkv, w_proj, w_up, w_down, norm_rows = params
    normed = layer_norm(residual, norm_rows[0], norm_rows[1])
    qkv_all = mat_f32(normed, w_qkv).astype(jnp.bfloat16)
    by_head = qkv_all.reshape(TOKENS, 3, HEADS, HEAD_DIM).transpose(1, 2, 0, 3)
    head_out = lax.map(head_attend, (by_head[0], by_head[1], by_head[2]))
    head_out = head_out.transpose(1, 0, 2).reshape(TOKENS, WIDTH)
    residual = (residual.astype(jnp.float32) + mat_f32(head_out, w_proj.reshape(WIDTH, WIDTH))).astype(jnp.bfloat16)
    normed = layer_norm(residual, norm_rows[2], norm_rows[3])
    hidden = jax.nn.gelu(mat_f32(normed, w_up), approximate=True).astype(jnp.bfloat16)
    return (residual.astype(jnp.float32) + mat_f32(hidden, w_down)).astype(jnp.bfloat16)


def reference(latents, hint_embed, in_qkv, in_proj, in_up, in_down, in_norm, out_qkv, out_proj, out_up, out_down, out_norm, zero_proj, hint_proj, skip_proj, final_norm, w_out):
    def in_step(residual, params):
        residual = transformer_block(residual, params)
        return residual, residual

    def out_step(residual, xs_pack):
        merged = mat_f32(jnp.concatenate([residual, xs_pack[6]], axis=-1), xs_pack[5]).astype(jnp.bfloat16)
        return transformer_block(merged, xs_pack[:5]), None

    ctrl_start = (latents.astype(jnp.float32) + mat_f32(hint_embed, hint_proj)).astype(jnp.bfloat16)
    base_params = (in_qkv[0], in_proj[0], in_up[0], in_down[0], in_norm[0])
    ctrl_params = (in_qkv[1], in_proj[1], in_up[1], in_down[1], in_norm[1])
    base_outs = lax.scan(in_step, latents, base_params)[1]
    ctrl_outs = lax.scan(in_step, ctrl_start, ctrl_params)[1]
    ctrl_res = jnp.einsum("bnd,bde->bne", ctrl_outs.astype(jnp.float32), zero_proj.astype(jnp.float32)).astype(jnp.bfloat16)
    sum_all = (base_outs.astype(jnp.float32) + ctrl_res.astype(jnp.float32)).astype(jnp.bfloat16)
    out_xs = (out_qkv, out_proj, out_up, out_down, out_norm, skip_proj, sum_all[:LAYERS][::-1])
    out_state = lax.scan(out_step, sum_all[LAYERS], out_xs)[0]
    normed = layer_norm(out_state, final_norm[0], final_norm[1])
    return mat_f32(normed, w_out).astype(jnp.bfloat16)
```

```python
import functools
import math

import jax
import jax.numpy as jnp
from jax import lax
from jax.experimental import pallas as pl
from jax.experimental.pallas import tpu as pltpu
from jax.sharding import PartitionSpec as P

EPS = 1e-6
BF = jnp.bfloat16
F32 = jnp.float32
MESH = pl.DeviceIdType.MESH
HEADS_PER_STEP = 4
GELU_C = math.sqrt(2.0 / math.pi)


def mat_f32(left_op, right_op):
    return jnp.dot(left_op, right_op, preferred_element_type=F32)


def layer_norm(values, norm_gain, norm_shift):
    wide_vals = values.astype(F32)
    centered = wide_vals - jnp.mean(wide_vals, axis=-1, keepdims=True)
    variance = jnp.mean(centered * centered, axis=-1, keepdims=True)
    normed = centered * lax.rsqrt(variance + EPS)
    return (normed * norm_gain.astype(F32) + norm_shift.astype(F32)).astype(BF)


def col_tiles(width, tile):
    return [(c, min(c + tile, width)) for c in range(0, width, tile)]


def norm_rows_into(dst, src, gain, shift):
    rows = dst.shape[0]
    for r in range(0, rows, 64):
        dst[r:r + 64, :] = layer_norm(src[r:r + 64, :], gain, shift)


class Block:
    def __init__(self, me, refs, heads):
        self.me = me
        self.__dict__.update(refs)
        self.rows, self.width = self.u.shape
        self.heads = heads
        self.hd = self.width // heads
        self.u_tiles = col_tiles(self.width, 512)
        self.kv_tiles = col_tiles(2 * self.width, 768)

    def remote(self, src, dst, send, recv, flip):
        peer = self.me + flip - 2 * flip * lax.rem(lax.div(self.me, flip), 2)
        return pltpu.make_async_remote_copy(
            src_ref=src, dst_ref=dst, send_sem=send, recv_sem=recv,
            device_id={"group": peer}, device_id_type=MESH)

    def u_copy(self, slot, c):
        lo, hi = self.u_tiles[c]
        return self.remote(self.u.at[:, lo:hi], self.uc.at[slot, :, lo:hi],
                           self.u_send.at[c], self.u_recv.at[slot, c], 2)

    def kv_copy(self, slot, which, c):
        lo, hi = self.kv_tiles[c]
        return self.remote(self.kv.at[slot, 2 * which, :, lo:hi],
                           self.kv.at[slot, 2 * which + 1, :, lo:hi],
                           self.kv_send.at[which, c], self.kv_recv.at[slot, which, c], 1)

    def project_kv(self, slot, which):
        for c, (lo, hi) in enumerate(self.kv_tiles):
            w = self.wqkv[:, self.width + lo:self.width + hi]
            self.kv[slot, 2 * which, :, lo:hi] = mat_f32(self.t[...], w).astype(BF)
            self.kv_copy(slot, which, c).start()

    def attend(self, slot, part):
        rows, width, hd = self.rows, self.width, self.hd
        scale = hd ** -0.5 * math.log2(math.e)
        win = 256
        lane = lax.broadcasted_iota(jnp.int32, (1, win), 1)

        def one_head(h):
            first = h * hd
            base = pl.multiple_of(jnp.minimum(first // 128, (width - win) // 128) * 128, 128)
            off = first - base
            inside = jnp.logical_and(lane >= off, lane < off + hd)
            keep = jnp.where(inside, 1.0, 0.0).astype(F32)
            q = self.q[:, pl.ds(base, win)] * keep.astype(BF)
            k = self.kv[slot, 2 * part:2 * part + 2, :, pl.ds(base, win)].reshape(2 * rows, win)
            v_base = pl.multiple_of(width + base, 128)
            v = self.kv[slot, 2 * part:2 * part + 2, :, pl.ds(v_base, win)].reshape(2 * rows, win)
            s = lax.dot_general(q, k, (((1,), (1,)), ((), ())), preferred_element_type=F32)
            m = jnp.max(s, axis=-1, keepdims=True)
            e = jnp.exp2((s - m) * scale)
            l = jnp.sum(e, axis=-1, keepdims=True)
            o = mat_f32(e.astype(BF), v)
            here = jnp.broadcast_to(inside, (rows, win))
            old = self.o[:, pl.ds(base, win)]
            if part == 0:
                self.m[h] = jnp.broadcast_to(m, (rows, 128))
                self.l[h] = jnp.broadcast_to(l, (rows, 128))
                self.o[:, pl.ds(base, win)] = jnp.where(here, o, old)
            else:
                m0, l0 = self.m[h], self.l[h]
                m1 = jnp.broadcast_to(m, (rows, 128))
                l1 = jnp.broadcast_to(l, (rows, 128))
                top = jnp.maximum(m0, m1)
                a0 = jnp.exp2((m0 - top) * scale)
                a1 = jnp.exp2((m1 - top) * scale)
                inv = 1.0 / (l0 * a0 + l1 * a1)
                a0, a1 = a0 * inv, a1 * inv
                a0 = jnp.concatenate([a0, a0], axis=1)
                a1 = jnp.concatenate([a1, a1], axis=1)
                self.o[:, pl.ds(base, win)] = jnp.where(here, old * a0 + o * a1, old)

        def step(g, carry):
            for d in range(HEADS_PER_STEP):
                one_head(g * HEADS_PER_STEP + d)
            return carry

        lax.fori_loop(0, self.heads // HEADS_PER_STEP, step, 0)

    def weight(self, idx, layer):
        return pltpu.make_async_copy(self.w_src[idx](layer), self.w_dst[idx], self.w_sem.at[idx])

    def refill(self, idx, layer, count):
        @pl.when(layer + 1 < count)
        def _():
            self.weight(idx, layer + 1).start()

    def run(self, i, count, filler, before_out, after_tile, out):
        p = lax.rem(i, 2)
        self.weight(0, i).wait()
        g1, b1 = self.norms[i, 0:1, :], self.norms[i, 1:2, :]
        norm_rows_into(self.t, self.u, g1, b1)
        self.project_kv(p, 0)
        self.q[...] = mat_f32(self.t[...], self.wqkv[:, :self.width]).astype(BF)
        for c in range(len(self.kv_tiles)):
            self.kv_copy(p, 0, c).wait_recv()
        self.attend(p, 0)
        filler()
        for c in range(len(self.u_tiles)):
            self.u_copy(p, c).wait_recv()
        norm_rows_into(self.t, self.uc.at[p], g1, b1)
        self.project_kv(p, 1)
        self.refill(0, i, count)
        for c in range(len(self.kv_tiles)):
            self.kv_copy(p, 1, c).wait_recv()
        self.attend(p, 1)
        for which in range(2):
            for c in range(len(self.kv_tiles)):
                self.kv_copy(p, which, c).wait_send()
        self.weight(1, i).wait()
        self.t[...] = self.o[...].astype(BF)
        for lo, hi in col_tiles(self.width, 512):
            attn = mat_f32(self.t[...], self.wo[:, lo:hi])
            self.u2[:, lo:hi] = (self.u[:, lo:hi].astype(F32) + attn).astype(BF)
        self.refill(1, i, count)
        norm_rows_into(self.t, self.u2, self.norms[i, 2:3, :], self.norms[i, 3:4, :])
        self.weight(2, i).wait()
        for lo, hi in col_tiles(self.hid.shape[1], 768):
            x = mat_f32(self.t[...], self.w1[:, lo:hi])
            g = 0.5 * x * (1.0 + jnp.tanh(GELU_C * (x + 0.044715 * (x * x * x))))
            self.hid[:, lo:hi] = g.astype(BF)
        self.refill(2, i, count)
        self.weight(3, i).wait()
        before_out()
        for c, (lo, hi) in enumerate(self.u_tiles):
            mlp = mat_f32(self.hid[...], self.w2[:, lo:hi])
            out[:, lo:hi] = (self.u2[:, lo:hi].astype(F32) + mlp).astype(BF)
            after_tile(c)
        self.refill(3, i, count)


def barrier(me, flips):
    sem = pltpu.get_barrier_semaphore()
    for flip in flips:
        peer = me + flip - 2 * flip * lax.rem(lax.div(me, flip), 2)
        pl.semaphore_signal(sem, inc=1, device_id={"group": peer}, device_id_type=MESH)
    pl.semaphore_wait(sem, len(flips))


COMMON = ("u", "u2", "uc", "t", "q", "kv", "o", "m", "l", "hid", "wqkv", "wo", "w1", "w2", "w_sem", "u_send", "u_recv", "kv_send", "kv_recv")


def common_scratch(rows, width, hidden, heads):
    u_n = len(col_tiles(width, 512))
    kv_n = len(col_tiles(2 * width, 768))
    return [
        pltpu.VMEM((rows, width), BF),
        pltpu.VMEM((rows, width), BF),
        pltpu.VMEM((2, rows, width), BF),
        pltpu.VMEM((rows, width), BF),
        pltpu.VMEM((rows, width), BF),
        pltpu.VMEM((2, 4, rows, 2 * width), BF),
        pltpu.VMEM((rows, width), F32),
        pltpu.VMEM((heads, rows, 128), F32),
        pltpu.VMEM((heads, rows, 128), F32),
        pltpu.VMEM((rows, hidden), BF),
        pltpu.VMEM((width, 3 * width), BF),
        pltpu.VMEM((width, width), BF),
        pltpu.VMEM((width, hidden), BF),
        pltpu.VMEM((hidden, width), BF),
        pltpu.SemaphoreType.DMA((5,)),
        pltpu.SemaphoreType.DMA((u_n,)),
        pltpu.SemaphoreType.DMA((2, u_n)),
        pltpu.SemaphoreType.DMA((2, kv_n)),
        pltpu.SemaphoreType.DMA((2, 2, kv_n)),
    ]


def in_kernel(heads, count, u0, norms, qkv_h, wo_h, w1_h, w2_h, wz_h, a_all, r_all, *scratch):
    refs = dict(zip(COMMON, scratch[:len(COMMON)]))
    wz, rbuf, r_send, r_recv, a_sem = scratch[len(COMMON):]
    me = lax.axis_index("group")
    branch = lax.div(me, 4)
    blk = Block(me, refs, heads)
    blk.norms = norms
    blk.w_src = [lambda i: qkv_h.at[branch, i], lambda i: wo_h.at[branch, i], lambda i: w1_h.at[branch, i],
                 lambda i: w2_h.at[branch, i], lambda i: wz_h.at[i]]
    blk.w_dst = [blk.wqkv, blk.wo, blk.w1, blk.w2, wz]
    for idx in range(4):
        blk.weight(idx, 0).start()

    @pl.when(branch == 1)
    def _():
        blk.weight(4, 0).start()

    blk.u[...] = u0[...]
    barrier(me, (1, 2, 4))
    for c in range(len(blk.u_tiles)):
        blk.u_copy(0, c).start()

    def a_store(i):
        return pltpu.make_async_copy(blk.u, a_all.at[i], a_sem)

    def r_copy(j):
        par = lax.rem(j, 2)
        return pltpu.make_async_remote_copy(
            src_ref=rbuf.at[par], dst_ref=r_all.at[j], send_sem=r_send.at[par], recv_sem=r_recv.at[j],
            device_id={"group": lax.rem(me, 4)}, device_id_type=MESH)

    def make_r(j):
        @pl.when(j >= 2)
        def _():
            r_copy(j - 2).wait_send()

        blk.weight(4, j).wait()
        par = lax.rem(j, 2)
        for lo, hi in col_tiles(blk.width, 512):
            rbuf[par, :, lo:hi] = mat_f32(blk.u[...], wz[:, lo:hi]).astype(BF)
        r_copy(j).start()
        blk.refill(4, j, count)

    def layer(i, carry):
        def filler():
            @pl.when(jnp.logical_and(branch == 1, i >= 1))
            def _():
                make_r(i - 1)

        def before_out():
            for c in range(len(blk.u_tiles)):
                blk.u_copy(0, c).wait_send()

            @pl.when(i >= 1)
            def _():
                a_store(i - 1).wait()

        def after_tile(c):
            @pl.when(i + 1 < count)
            def _():
                blk.u_copy(1 - lax.rem(i, 2), c).start()

        blk.run(i, count, filler, before_out, after_tile, blk.u)
        a_store(i).start()
        return carry

    lax.fori_loop(0, count, layer, 0)

    @pl.when(branch == 1)
    def _():
        make_r(jnp.int32(count - 1))
        if count >= 2:
            r_copy(jnp.int32(count - 2)).wait_send()
        r_copy(jnp.int32(count - 1)).wait_send()

    @pl.when(branch == 0)
    def _():
        def take(j, carry):
            r_copy(j).wait_recv()
            return carry
        lax.fori_loop(0, count, take, 0)

    a_store(count - 1).wait()


def out_kernel(heads, count, a_all, r_all, norms, qkv_h, wo_h, w1_h, w2_h, ws_h, y, *scratch):
    refs = dict(zip(COMMON, scratch[:len(COMMON)]))
    ws, pair, sa, sr, s_sem = scratch[len(COMMON):]
    me = lax.axis_index("group")

    def skip_load(j):
        idx = count - j
        return (pltpu.make_async_copy(a_all.at[idx], sa, s_sem.at[0]),
                pltpu.make_async_copy(r_all.at[idx], sr, s_sem.at[1]))

    def run_all():
        blk = Block(me, refs, heads)
        width = blk.width
        blk.norms = norms
        blk.w_src = [lambda i: qkv_h.at[i], lambda i: wo_h.at[i], lambda i: w1_h.at[i], lambda i: w2_h.at[i],
                     lambda i: ws_h.at[i]]
        blk.w_dst = [blk.wqkv, blk.wo, blk.w1, blk.w2, ws]
        for idx in (4, 0, 1, 2, 3):
            blk.weight(idx, 0).start()
        for cp in skip_load(0):
            cp.start()
        barrier(me, (1, 2))
        for cp in skip_load(0):
            cp.wait()
        pair[:, :width] = (sa[...].astype(F32) + sr[...].astype(F32)).astype(BF)
        for cp in skip_load(1):
            cp.start()

        def layer(i, carry):
            for cp in skip_load(i + 1):
                cp.wait()
            pair[:, width:] = (sa[...].astype(F32) + sr[...].astype(F32)).astype(BF)

            @pl.when(i + 1 < count)
            def _():
                for cp in skip_load(i + 2):
                    cp.start()

            blk.weight(4, i).wait()
            for c, (lo, hi) in enumerate(blk.u_tiles):
                blk.u[:, lo:hi] = mat_f32(pair[...], ws[:, lo:hi]).astype(BF)
                blk.u_copy(lax.rem(i, 2), c).start()
            blk.refill(4, i, count)

            def before_out():
                for c in range(len(blk.u_tiles)):
                    blk.u_copy(0, c).wait_send()

            blk.run(i, count, lambda: None, before_out, lambda c: None, pair.at[:, :width])
            return carry

        lax.fori_loop(0, count, layer, 0)
        y[...] = pair[:, :width]

    pl.when(lax.div(me, 4) == 0)(run_all)


def any_spec():
    return pl.BlockSpec(memory_space=pl.ANY)


def vmem_spec():
    return pl.BlockSpec(memory_space=pltpu.VMEM)


def solution(mesh):
    group_size = mesh.shape["group"]
    half_size = group_size // 2
    swap_perm = [(dev_id, (dev_id + half_size) % group_size) for dev_id in range(group_size)]
    to_ctrl = [(dev_id, dev_id + half_size) for dev_id in range(half_size)]

    def device_step(x_own, hint_own, in_qkv, in_proj, in_up, in_down, in_norm, out_qkv, out_proj, out_up, out_down, out_norm, zero_proj, hint_proj, skip_proj, final_norm, w_out):
        n_in, n_out = zero_proj.shape[0], skip_proj.shape[0]
        tok_own, width = x_own.shape
        rows = 2 * tok_own
        hidden = in_up.shape[-1]
        heads = in_proj.shape[2]
        branch = lax.axis_index("group") // half_size
        is_base = branch == 0
        x_other = lax.ppermute(x_own, "group", swap_perm)
        hint_recv = lax.ppermute(hint_own, "group", to_ctrl)
        x_local = jnp.where(is_base, jnp.concatenate([x_own, x_other], axis=0), jnp.concatenate([x_other, x_own], axis=0))
        hint_local = jnp.where(is_base, jnp.zeros((rows, width), BF), jnp.concatenate([hint_recv, hint_own], axis=0))
        u0 = (x_local.astype(F32) + mat_f32(hint_local, hint_proj)).astype(BF)
        norms = lax.dynamic_index_in_dim(in_norm, branch, 0, keepdims=False).astype(F32)
        params = dict(vmem_limit_bytes=67_000_000, has_side_effects=True)
        a_all, r_all = pl.pallas_call(
            functools.partial(in_kernel, heads, n_in),
            name="in_phase",
            out_shape=[jax.ShapeDtypeStruct((n_in, rows, width), BF)] * 2,
            in_specs=[vmem_spec(), vmem_spec()] + [any_spec()] * 5,
            out_specs=[any_spec(), any_spec()],
            scratch_shapes=common_scratch(rows, width, hidden, heads) + [
                pltpu.VMEM((width, width), BF),
                pltpu.VMEM((2, rows, width), BF),
                pltpu.SemaphoreType.DMA((2,)),
                pltpu.SemaphoreType.DMA((n_in,)),
                pltpu.SemaphoreType.DMA,
            ],
            compiler_params=pltpu.CompilerParams(collective_id=0, **params),
        )(u0, norms, in_qkv, in_proj.reshape(2, n_in, width, width), in_up, in_down, zero_proj)
        o_n = pl.pallas_call(
            functools.partial(out_kernel, heads, n_out),
            name="out_phase",
            out_shape=jax.ShapeDtypeStruct((rows, width), BF),
            in_specs=[any_spec()] * 2 + [vmem_spec()] + [any_spec()] * 5,
            out_specs=vmem_spec(),
            scratch_shapes=common_scratch(rows, width, hidden, heads) + [
                pltpu.VMEM((2 * width, width), BF),
                pltpu.VMEM((rows, 2 * width), BF),
                pltpu.VMEM((rows, width), BF),
                pltpu.VMEM((rows, width), BF),
                pltpu.SemaphoreType.DMA((2,)),
            ],
            compiler_params=pltpu.CompilerParams(collective_id=1, **params),
        )(a_all, r_all, out_norm.astype(F32), out_qkv, out_proj.reshape(n_out, width, width), out_up, out_down, skip_proj)
        y_local = mat_f32(layer_norm(o_n, final_norm[0], final_norm[1]), w_out).astype(BF)
        y_recv = lax.ppermute(y_local[tok_own:], "group", to_ctrl)
        return jnp.where(is_base, y_local[:tok_own], y_recv)

    tok_spec = P(("data", "group"), None)
    return jax.shard_map(device_step, mesh=mesh, in_specs=(tok_spec, tok_spec) + (P(),) * 15, out_specs=tok_spec, check_vma=False)
```

```python
import functools
import math

import jax
import jax.numpy as jnp
from jax import lax
from jax.experimental import pallas as pl
from jax.experimental.pallas import tpu as pltpu
from jax.sharding import PartitionSpec as P

EPS = 1e-6
BF = jnp.bfloat16
F32 = jnp.float32
MESH = pl.DeviceIdType.MESH
HEADS_PER_STEP = 4
U_TILE = 512
KV_TILE = 768
GELU_C = math.sqrt(2.0 / math.pi)


def mat_f32(left_op, right_op):
    return jnp.dot(left_op, right_op, preferred_element_type=F32)


def layer_norm(values, norm_gain, norm_shift):
    wide_vals = values.astype(F32)
    centered = wide_vals - jnp.mean(wide_vals, axis=-1, keepdims=True)
    variance = jnp.mean(centered * centered, axis=-1, keepdims=True)
    normed = centered * lax.rsqrt(variance + EPS)
    return (normed * norm_gain.astype(F32) + norm_shift.astype(F32)).astype(BF)


def col_tiles(width, tile):
    return [(c, min(c + tile, width)) for c in range(0, width, tile)]


def norm_rows_into(dst, src, lo, rows, gain, shift):
    for r in range(0, rows, 32):
        at = pl.ds(pl.multiple_of(lo + r, 32), 32)
        dst[at, :] = layer_norm(src[at, :], gain, shift)


def flipped(me, flip):
    return me + flip - 2 * flip * lax.rem(lax.div(me, flip), 2)


class Block:
    def __init__(self, me, refs, heads):
        self.me = me
        self.__dict__.update(refs)
        self.rows, self.width = self.u.shape
        self.heads = heads
        self.hd = self.width // heads
        self.half = self.rows // 2
        self.u_tiles = col_tiles(self.width, U_TILE)
        self.kv_tiles = col_tiles(2 * self.width, KV_TILE)

    def group(self, g):
        return pl.ds(pl.multiple_of(g * self.half, self.half), self.half)

    def remote(self, src, dst, send, recv, flip):
        return pltpu.make_async_remote_copy(
            src_ref=src, dst_ref=dst, send_sem=send, recv_sem=recv,
            device_id={"group": flipped(self.me, flip)}, device_id_type=MESH)

    def u_copy(self, slot, g, c):
        (lo, hi), at = self.u_tiles[c], self.group(g)
        return self.remote(self.u.at[at, lo:hi], self.uc.at[slot, at, lo:hi],
                           self.u_send.at[g, c], self.u_recv.at[slot, g, c], 2)

    def kv_copy(self, slot, g, c):
        lo, hi = self.kv_tiles[c]
        part, at, sem = (0, pl.ds(0, self.rows), 0) if g is None else (2, self.group(g), 1 + g)
        return self.remote(self.kv.at[slot, part, at, lo:hi],
                           self.kv.at[slot, part + 1, at, lo:hi],
                           self.kv_send.at[sem, c], self.kv_recv.at[slot, sem, c], 1)

    def project_kv(self, slot, g):
        part, at = (0, pl.ds(0, self.rows)) if g is None else (2, self.group(g))
        for c, (lo, hi) in enumerate(self.kv_tiles):
            w = self.wqkv[:, self.width + lo:self.width + hi]
            self.kv[slot, part, at, lo:hi] = mat_f32(self.t[at, :], w).astype(BF)
            self.kv_copy(slot, g, c).start()

    def attend(self, slot, part, lo, hi):
        rows, width, hd = self.rows, self.width, self.hd
        scale = hd ** -0.5 * math.log2(math.e)
        win = 256
        lane = lax.broadcasted_iota(jnp.int32, (1, win), 1)

        def place(h):
            first = h * hd
            base = pl.multiple_of(jnp.minimum(first // 128, (width - win) // 128) * 128, 128)
            off = first - base
            return base, jnp.logical_and(lane >= off, lane < off + hd)

        def scores(h):
            base, inside = place(h)
            keep = jnp.where(inside, 1.0, 0.0).astype(F32)
            q = self.q[:, pl.ds(base, win)] * keep.astype(BF)
            k = self.kv[slot, 2 * part:2 * part + 2, :, pl.ds(base, win)].reshape(2 * rows, win)
            return lax.dot_general(q, k, (((1,), (1,)), ((), ())), preferred_element_type=F32)

        def finish(h, s):
            base, inside = place(h)
            v_base = pl.multiple_of(width + base, 128)
            v = self.kv[slot, 2 * part:2 * part + 2, :, pl.ds(v_base, win)].reshape(2 * rows, win)
            m = jnp.max(s, axis=-1, keepdims=True)
            e = jnp.exp2((s - m) * scale)
            l = jnp.sum(e, axis=-1, keepdims=True)
            o = mat_f32(e.astype(BF), v)
            here = jnp.broadcast_to(inside, (rows, win))
            old = self.o[:, pl.ds(base, win)]
            if part == 0:
                self.m[h] = jnp.broadcast_to(m, (rows, 128))
                self.l[h] = jnp.broadcast_to(l, (rows, 128))
                self.o[:, pl.ds(base, win)] = jnp.where(here, o, old)
            else:
                m0, l0 = self.m[h], self.l[h]
                m1 = jnp.broadcast_to(m, (rows, 128))
                l1 = jnp.broadcast_to(l, (rows, 128))
                top = jnp.maximum(m0, m1)
                a0 = jnp.exp2((m0 - top) * scale)
                a1 = jnp.exp2((m1 - top) * scale)
                inv = 1.0 / (l0 * a0 + l1 * a1)
                a0, a1 = a0 * inv, a1 * inv
                a0 = jnp.concatenate([a0, a0], axis=1)
                a1 = jnp.concatenate([a1, a1], axis=1)
                self.o[:, pl.ds(base, win)] = jnp.where(here, old * a0 + o * a1, old)

        def step(at, carry):
            h0 = at * HEADS_PER_STEP
            s = scores(h0)
            for d in range(HEADS_PER_STEP):
                nxt = scores(h0 + d + 1) if d + 1 < HEADS_PER_STEP else None
                finish(h0 + d, s)
                s = nxt
            return carry

        lax.fori_loop(lo, hi, step, 0)

    def weight(self, idx, layer):
        return pltpu.make_async_copy(self.w_src[idx](layer), self.w_dst[idx], self.w_sem.at[idx])

    def refill(self, idx, layer, count):
        @pl.when(layer + 1 < count)
        def _():
            self.weight(idx, layer + 1).start()

    def run(self, i, count, filler, before_out, put):
        p = lax.rem(i, 2)
        n = self.norm_of(i)
        g1, b1, g2, b2 = n[0:1, :], n[1:2, :], n[2:3, :], n[3:4, :]
        every_kv, every_u = range(len(self.kv_tiles)), range(len(self.u_tiles))
        self.weight(0, i).wait()
        norm_rows_into(self.t, self.u, 0, self.rows, g1, b1)
        self.project_kv(p, None)
        self.q[...] = mat_f32(self.t[...], self.wqkv[:, :self.width]).astype(BF)
        for c in every_kv:
            self.kv_copy(p, None, c).wait_recv()

        def gather(g, carry):
            steps = self.heads // HEADS_PER_STEP // 2
            self.attend(p, 0, g * steps, (g + 1) * steps)
            for c in every_u:
                self.u_copy(p, g, c).wait_recv()
            norm_rows_into(self.t, self.uc.at[p], g * self.half, self.half, g1, b1)
            self.project_kv(p, g)
            return carry

        lax.fori_loop(0, 2, gather, 0)
        self.refill(0, i, count)
        filler()
        for g in range(2):
            for c in every_kv:
                self.kv_copy(p, g, c).wait_recv()
        self.attend(p, 1, 0, self.heads // HEADS_PER_STEP)
        for g in (None, 0, 1):
            for c in every_kv:
                self.kv_copy(p, g, c).wait_send()
        for idx in (1, 2, 3):
            self.weight(idx, i).wait()
        before_out()

        def finish(g, carry):
            at = self.group(g)
            self.t[at, :] = self.o[at, :].astype(BF)
            for lo, hi in col_tiles(self.width, 512):
                attn = mat_f32(self.t[at, :], self.wo[:, lo:hi])
                self.u2[at, lo:hi] = (self.u[at, lo:hi].astype(F32) + attn).astype(BF)
            norm_rows_into(self.t, self.u2, g * self.half, self.half, g2, b2)
            for lo, hi in col_tiles(self.hid.shape[1], 768):
                x = mat_f32(self.t[at, :], self.w1[:, lo:hi])
                gl = 0.5 * x * (1.0 + jnp.tanh(GELU_C * (x + 0.044715 * (x * x * x))))
                self.hid[:, lo:hi] = gl.astype(BF)
            for c in every_u:
                self.u_copy(0, g, c).wait_send()
            for c, (lo, hi) in enumerate(self.u_tiles):
                mlp = mat_f32(self.hid[...], self.w2[:, lo:hi])
                put(g, c, (self.u2[at, lo:hi].astype(F32) + mlp).astype(BF))
            return carry

        lax.fori_loop(0, 2, finish, 0)
        for idx in (1, 2, 3):
            self.refill(idx, i, count)


def barrier(me, flips):
    sem = pltpu.get_barrier_semaphore()
    for flip in flips:
        pl.semaphore_signal(sem, inc=1, device_id={"group": flipped(me, flip)}, device_id_type=MESH)
    pl.semaphore_wait(sem, len(flips))


COMMON = ("u", "u2", "uc", "t", "q", "kv", "o", "m", "l", "hid", "wqkv", "wo", "w1", "w2", "w_sem", "u_send", "u_recv", "kv_send", "kv_recv")


def common_scratch(rows, width, hidden, heads):
    u_n = len(col_tiles(width, U_TILE))
    kv_n = len(col_tiles(2 * width, KV_TILE))
    return [
        pltpu.VMEM((rows, width), BF),
        pltpu.VMEM((rows, width), BF),
        pltpu.VMEM((2, rows, width), BF),
        pltpu.VMEM((rows, width), BF),
        pltpu.VMEM((rows, width), BF),
        pltpu.VMEM((2, 4, rows, 2 * width), BF),
        pltpu.VMEM((rows, width), F32),
        pltpu.VMEM((heads, rows, 128), F32),
        pltpu.VMEM((heads, rows, 128), F32),
        pltpu.VMEM((rows // 2, hidden), BF),
        pltpu.VMEM((width, 3 * width), BF),
        pltpu.VMEM((width, width), BF),
        pltpu.VMEM((width, hidden), BF),
        pltpu.VMEM((hidden, width), BF),
        pltpu.SemaphoreType.DMA((6,)),
        pltpu.SemaphoreType.DMA((2, u_n)),
        pltpu.SemaphoreType.DMA((2, 2, u_n)),
        pltpu.SemaphoreType.DMA((3, kv_n)),
        pltpu.SemaphoreType.DMA((2, 3, kv_n)),
    ]


def in_kernel(heads, count, x_own, h_own, norms, hp_h, qkv_h, wo_h, w1_h, w2_h, wz_h, a_all, r_all, *scratch):
    refs = dict(zip(COMMON, scratch[:len(COMMON)]))
    wz, rbuf, r_send, r_recv, a_sem, x_sem = scratch[len(COMMON):]
    me = lax.axis_index("group")
    branch = lax.div(me, 4)
    blk = Block(me, refs, heads)
    blk.norm_of = lambda i: norms[branch, i].astype(F32)
    blk.w_src = [lambda i: qkv_h.at[branch, i], lambda i: wo_h.at[branch, i], lambda i: w1_h.at[branch, i],
                 lambda i: w2_h.at[branch, i], lambda i: wz_h.at[i]]
    blk.w_dst = [blk.wqkv, blk.wo, blk.w1, blk.w2, wz]
    hint_w = pltpu.make_async_copy(hp_h, wz, blk.w_sem.at[5])
    hint_w.start()
    for idx in range(4):
        blk.weight(idx, 0).start()
    barrier(me, (1, 2, 4))
    own = x_own.shape[0]

    give = blk.remote(blk.u2.at[0:own, :], blk.u.at[pl.ds(pl.multiple_of(branch * own, own), own), :],
                      x_sem.at[0], x_sem.at[1], 4)
    hint_w.wait()
    mine = pl.ds(pl.multiple_of(branch * own, own), own)
    for lo, hi in col_tiles(blk.width, 512):
        x = x_own[:, lo:hi]
        ctrl = (x.astype(F32) + mat_f32(h_own[...], wz[:, lo:hi])).astype(BF)
        blk.t[0:own, lo:hi] = ctrl

    @pl.when(branch == 0)
    def _():
        blk.u2[0:own, :] = blk.t[0:own, :]
        blk.u[mine, :] = x_own[...]

    @pl.when(branch == 1)
    def _():
        blk.u2[0:own, :] = x_own[...]
        blk.u[mine, :] = blk.t[0:own, :]
        blk.weight(4, 0).start()

    give.start()
    give.wait()
    for g in range(2):
        for c in range(len(blk.u_tiles)):
            blk.u_copy(0, g, c).start()

    def a_store(i):
        return pltpu.make_async_copy(blk.u, a_all.at[i], a_sem)

    def r_copy(j):
        par = lax.rem(j, 2)
        return pltpu.make_async_remote_copy(
            src_ref=rbuf.at[par], dst_ref=r_all.at[j], send_sem=r_send.at[par], recv_sem=r_recv.at[j],
            device_id={"group": lax.rem(me, 4)}, device_id_type=MESH)

    def make_r(j):
        @pl.when(j >= 2)
        def _():
            r_copy(j - 2).wait_send()

        blk.weight(4, j).wait()
        par = lax.rem(j, 2)
        for lo, hi in col_tiles(blk.width, 512):
            rbuf[par, :, lo:hi] = mat_f32(blk.u[...], wz[:, lo:hi]).astype(BF)
        r_copy(j).start()
        blk.refill(4, j, count)

    def layer(i, carry):
        def filler():
            @pl.when(jnp.logical_and(branch == 1, i >= 1))
            def _():
                make_r(i - 1)

        def before_out():
            @pl.when(i >= 1)
            def _():
                a_store(i - 1).wait()

        def put(g, c, values):
            lo, hi = blk.u_tiles[c]
            blk.u[blk.group(g), lo:hi] = values

            @pl.when(i + 1 < count)
            def _():
                blk.u_copy(1 - lax.rem(i, 2), g, c).start()

        blk.run(i, count, filler, before_out, put)
        a_store(i).start()
        return carry

    lax.fori_loop(0, count, layer, 0)

    @pl.when(branch == 1)
    def _():
        make_r(jnp.int32(count - 1))
        if count >= 2:
            r_copy(jnp.int32(count - 2)).wait_send()
        r_copy(jnp.int32(count - 1)).wait_send()

    @pl.when(branch == 0)
    def _():
        def take(j, carry):
            r_copy(j).wait_recv()
            return carry
        lax.fori_loop(0, count, take, 0)

    a_store(count - 1).wait()


def out_kernel(heads, count, a_all, r_all, norms, fin, qkv_h, wo_h, w1_h, w2_h, ws_h, wf_h, y, *scratch):
    refs = dict(zip(COMMON, scratch[:len(COMMON)]))
    top, low_w, low, o16, sa, sr, s_sem, y_sem = scratch[len(COMMON):]
    me = lax.axis_index("group")
    branch = lax.div(me, 4)
    own = y.shape[0]
    blk = Block(me, refs, heads)
    width = blk.width
    give = blk.remote(blk.u2.at[own:2 * own, :], y, y_sem.at[0], y_sem.at[1], 4)
    blk.norm_of = lambda i: norms[i].astype(F32)
    blk.w_src = [lambda i: qkv_h.at[i], lambda i: wo_h.at[i], lambda i: w1_h.at[i], lambda i: w2_h.at[i],
                 lambda i: ws_h.at[i, 0:width, :], lambda i: ws_h.at[i, width:2 * width, :]]
    blk.w_dst = [blk.wqkv, blk.wo, blk.w1, blk.w2, top, low_w]
    last_w = pltpu.make_async_copy(wf_h, blk.wo, blk.w_sem.at[1])

    def skip_load(j):
        idx = count - j
        return (pltpu.make_async_copy(a_all.at[idx], sa, s_sem.at[0]),
                pltpu.make_async_copy(r_all.at[idx], sr, s_sem.at[1]))

    def skip_sum(dst):
        for r in range(0, blk.rows, 32):
            dst[r:r + 32, :] = (sa[r:r + 32, :].astype(F32) + sr[r:r + 32, :].astype(F32)).astype(BF)

    def make_low(j):
        for cp in skip_load(j + 1):
            cp.wait()
        skip_sum(blk.t)

        @pl.when(j + 1 < count)
        def _():
            for cp in skip_load(j + 2):
                cp.start()

        blk.weight(5, j).wait()
        for lo, hi in col_tiles(width, 512):
            low[:, lo:hi] = mat_f32(blk.t[...], low_w[:, lo:hi])
        blk.refill(5, j, count)

    def merge(g, slot):
        at = blk.group(g)
        for c, (lo, hi) in enumerate(blk.u_tiles):
            blk.u[at, lo:hi] = (low[at, lo:hi] + mat_f32(o16[at, :], top[:, lo:hi])).astype(BF)
            blk.u_copy(slot, g, c).start()

    def run_all():
        for idx in (5, 4, 0, 1, 2, 3):
            blk.weight(idx, 0).start()
        for cp in skip_load(0):
            cp.start()
        barrier(me, (1, 2, 4))
        for cp in skip_load(0):
            cp.wait()
        skip_sum(o16)
        for cp in skip_load(1):
            cp.start()
        make_low(0)
        blk.weight(4, 0).wait()
        lax.fori_loop(0, 2, lambda g, carry: merge(g, 0) or carry, 0)
        blk.refill(4, 0, count)

        def layer(i, carry):
            def filler():
                @pl.when(i + 1 < count)
                def _():
                    make_low(i + 1)

            def before_out():
                @pl.when(i + 1 < count)
                def _():
                    blk.weight(4, i + 1).wait()

            def put(g, c, values):
                lo, hi = blk.u_tiles[c]
                o16[blk.group(g), lo:hi] = values
                if c == len(blk.u_tiles) - 1:
                    @pl.when(i + 1 < count)
                    def _():
                        merge(g, 1 - lax.rem(i, 2))

            blk.run(i, count, filler, before_out, put)
            blk.refill(4, i + 1, count)
            return carry

        lax.fori_loop(0, count, layer, 0)
        last_w.start()
        norm_rows_into(blk.t, o16, 0, blk.rows, fin[0:1, :].astype(F32), fin[1:2, :].astype(F32))
        last_w.wait()
        for r0, r1 in ((own, 2 * own), (0, own)):
            for lo, hi in col_tiles(width, 512):
                blk.u2[r0:r1, lo:hi] = mat_f32(blk.t[r0:r1, :], blk.wo[:, lo:hi]).astype(BF)
            if r0 > 0:
                give.start()
        y[...] = blk.u2[0:own, :]
        give.wait_send()

    pl.when(branch == 0)(run_all)

    @pl.when(branch == 1)
    def _():
        barrier(me, (4,))
        give.wait_recv()


def any_spec():
    return pl.BlockSpec(memory_space=pl.ANY)


def vmem_spec():
    return pl.BlockSpec(memory_space=pltpu.VMEM)


def solution(mesh):
    def device_step(x_own, hint_own, in_qkv, in_proj, in_up, in_down, in_norm, out_qkv, out_proj, out_up, out_down, out_norm, zero_proj, hint_proj, skip_proj, final_norm, w_out):
        n_in, n_out = zero_proj.shape[0], skip_proj.shape[0]
        tok_own, width = x_own.shape
        rows = 2 * tok_own
        hidden = in_up.shape[-1]
        heads = in_proj.shape[2]
        params = dict(vmem_limit_bytes=67_000_000, has_side_effects=True)
        a_all, r_all = pl.pallas_call(
            functools.partial(in_kernel, heads, n_in),
            name="in_phase",
            out_shape=[jax.ShapeDtypeStruct((n_in, rows, width), BF)] * 2,
            in_specs=[vmem_spec()] * 3 + [any_spec()] * 6,
            out_specs=[any_spec(), any_spec()],
            scratch_shapes=common_scratch(rows, width, hidden, heads) + [
                pltpu.VMEM((width, width), BF),
                pltpu.VMEM((2, rows, width), BF),
                pltpu.SemaphoreType.DMA((2,)),
                pltpu.SemaphoreType.DMA((n_in,)),
                pltpu.SemaphoreType.DMA,
                pltpu.SemaphoreType.DMA((2,)),
            ],
            compiler_params=pltpu.CompilerParams(collective_id=0, **params),
        )(x_own, hint_own, in_norm, hint_proj, in_qkv, in_proj.reshape(2, n_in, width, width), in_up, in_down, zero_proj)
        return pl.pallas_call(
            functools.partial(out_kernel, heads, n_out),
            name="out_phase",
            out_shape=jax.ShapeDtypeStruct((tok_own, width), BF),
            in_specs=[any_spec()] * 2 + [vmem_spec()] * 2 + [any_spec()] * 6,
            out_specs=vmem_spec(),
            scratch_shapes=common_scratch(rows, width, hidden, heads) + [
                pltpu.VMEM((width, width), BF),
                pltpu.VMEM((width, width), BF),
                pltpu.VMEM((rows, width), F32),
                pltpu.VMEM((rows, width), BF),
                pltpu.VMEM((rows, width), BF),
                pltpu.VMEM((rows, width), BF),
                pltpu.SemaphoreType.DMA((2,)),
                pltpu.SemaphoreType.DMA((2,)),
            ],
            compiler_params=pltpu.CompilerParams(collective_id=1, **params),
        )(a_all, r_all, out_norm, final_norm, out_qkv, out_proj.reshape(n_out, width, width), out_up, out_down, skip_proj, w_out)

    tok_spec = P(("data", "group"), None)
    return jax.shard_map(device_step, mesh=mesh, in_specs=(tok_spec, tok_spec) + (P(),) * 15, out_specs=tok_spec, check_vma=False)
```

```python
import functools
import math

import jax
import jax.numpy as jnp
from jax import lax
from jax.experimental import pallas as pl
from jax.experimental.pallas import tpu as pltpu
from jax.sharding import PartitionSpec as P

EPS = 1e-6
BF = jnp.bfloat16
F32 = jnp.float32
MESH = pl.DeviceIdType.MESH
HEADS_PER_STEP = 8
U_TILE = 512
KV_TILE = 768
GELU_C = math.sqrt(2.0 / math.pi)


def mat_f32(left_op, right_op):
    return jnp.dot(left_op, right_op, preferred_element_type=F32)


def layer_norm(values, norm_gain, norm_shift):
    wide_vals = values.astype(F32)
    centered = wide_vals - jnp.mean(wide_vals, axis=-1, keepdims=True)
    variance = jnp.mean(centered * centered, axis=-1, keepdims=True)
    normed = centered * lax.rsqrt(variance + EPS)
    return (normed * norm_gain.astype(F32) + norm_shift.astype(F32)).astype(BF)


def col_tiles(width, tile):
    return [(c, min(c + tile, width)) for c in range(0, width, tile)]


def norm_rows_into(dst, src, lo, rows, gain, shift):
    for r in range(0, rows, 32):
        at = pl.ds(pl.multiple_of(lo + r, 32), 32)
        dst[at, :] = layer_norm(src[at, :], gain, shift)


def flipped(me, flip):
    return me + flip - 2 * flip * lax.rem(lax.div(me, flip), 2)


class Block:
    def __init__(self, me, refs, heads):
        self.me = me
        self.__dict__.update(refs)
        self.rows, self.width = self.u.shape
        self.heads = heads
        self.hd = self.width // heads
        self.half = self.rows // 2
        self.u_tiles = col_tiles(self.width, U_TILE)
        self.kv_tiles = col_tiles(2 * self.width, KV_TILE)

    def group(self, g):
        return pl.ds(pl.multiple_of(g * self.half, self.half), self.half)

    def remote(self, src, dst, send, recv, flip):
        return pltpu.make_async_remote_copy(
            src_ref=src, dst_ref=dst, send_sem=send, recv_sem=recv,
            device_id={"group": flipped(self.me, flip)}, device_id_type=MESH)

    def u_copy(self, slot, g, c):
        (lo, hi), at = self.u_tiles[c], self.group(g)
        return self.remote(self.u.at[at, lo:hi], self.uc.at[slot, at, lo:hi],
                           self.u_send.at[g, c], self.u_recv.at[slot, g, c], 2)

    def kv_copy(self, slot, g, c):
        lo, hi = self.kv_tiles[c]
        part, at, sem = (0, pl.ds(0, self.rows), 0) if g is None else (2, self.group(g), 1 + g)
        return self.remote(self.kv.at[slot, part, at, lo:hi],
                           self.kv.at[slot, part + 1, at, lo:hi],
                           self.kv_send.at[sem, c], self.kv_recv.at[slot, sem, c], 1)

    def project_kv(self, slot, g):
        part, at = (0, pl.ds(0, self.rows)) if g is None else (2, self.group(g))
        for c, (lo, hi) in enumerate(self.kv_tiles):
            w = self.wqkv[:, self.width + lo:self.width + hi]
            self.kv[slot, part, at, lo:hi] = mat_f32(self.t[at, :], w).astype(BF)
            self.kv_copy(slot, g, c).start()

    def attend(self, slot, part, lo, hi):
        rows, width, hd = self.rows, self.width, self.hd
        chip, at = (0, pl.ds(0, rows)) if part == 0 else (2, self.group(part - 1))
        keys = 2 * at.size
        scale = hd ** -0.5 * math.log2(math.e)
        win = 256
        lane = lax.broadcasted_iota(jnp.int32, (1, win), 1)

        def place(h):
            first = h * hd
            base = pl.multiple_of(jnp.minimum(first // 128, (width - win) // 128) * 128, 128)
            off = first - base
            return base, jnp.logical_and(lane >= off, lane < off + hd)

        def scores(h):
            base, inside = place(h)
            keep = jnp.where(inside, 1.0, 0.0).astype(F32)
            q = self.q[:, pl.ds(base, win)] * keep.astype(BF)
            k = self.kv[slot, chip:chip + 2, at, pl.ds(base, win)].reshape(keys, win)
            return lax.dot_general(q, k, (((1,), (1,)), ((), ())), preferred_element_type=F32)

        def finish(h, s):
            base, inside = place(h)
            v_base = pl.multiple_of(width + base, 128)
            v = self.kv[slot, chip:chip + 2, at, pl.ds(v_base, win)].reshape(keys, win)
            m = jnp.max(s, axis=-1, keepdims=True) * scale
            e = jnp.exp2(s * scale - m)
            l = jnp.sum(e, axis=-1, keepdims=True)
            o = mat_f32(e.astype(BF), v)
            here = jnp.broadcast_to(inside, (rows, win))
            old = self.o[:, pl.ds(base, win)]
            if part == 0:
                self.m[h] = jnp.broadcast_to(m, (rows, 128))
                self.l[h] = jnp.broadcast_to(l, (rows, 128))
                self.o[:, pl.ds(base, win)] = jnp.where(here, o, old)
            else:
                m0, l0 = self.m[h], self.l[h]
                m1 = jnp.broadcast_to(m, (rows, 128))
                l1 = jnp.broadcast_to(l, (rows, 128))
                top = jnp.maximum(m0, m1)
                a0 = jnp.exp2(m0 - top)
                a1 = jnp.exp2(m1 - top)
                total = l0 * a0 + l1 * a1
                if part == 1:
                    self.m[h], self.l[h] = top, total
                else:
                    inv = 1.0 / total
                    a0, a1 = a0 * inv, a1 * inv
                a0 = jnp.concatenate([a0, a0], axis=1)
                a1 = jnp.concatenate([a1, a1], axis=1)
                self.o[:, pl.ds(base, win)] = jnp.where(here, old * a0 + o * a1, old)

        def step(at, carry):
            h0 = at * HEADS_PER_STEP
            s = scores(h0)
            for d in range(HEADS_PER_STEP):
                nxt = scores(h0 + d + 1) if d + 1 < HEADS_PER_STEP else None
                finish(h0 + d, s)
                s = nxt
            return carry

        lax.fori_loop(lo, hi, step, 0)

    def weight(self, idx, layer):
        return pltpu.make_async_copy(self.w_src[idx](layer), self.w_dst[idx], self.w_sem.at[idx])

    def refill(self, idx, layer, count):
        @pl.when(layer + 1 < count)
        def _():
            self.weight(idx, layer + 1).start()

    def run(self, i, count, filler, before_out, put):
        p = lax.rem(i, 2)
        n = self.norm_of(i)
        g1, b1, g2, b2 = n[0:1, :], n[1:2, :], n[2:3, :], n[3:4, :]
        every_kv, every_u = range(len(self.kv_tiles)), range(len(self.u_tiles))
        self.weight(0, i).wait()
        norm_rows_into(self.t, self.u, 0, self.rows, g1, b1)
        self.project_kv(p, None)
        self.q[...] = mat_f32(self.t[...], self.wqkv[:, :self.width]).astype(BF)
        for c in every_kv:
            self.kv_copy(p, None, c).wait_recv()

        def gather(g, carry):
            steps = self.heads // HEADS_PER_STEP // 2
            self.attend(p, 0, g * steps, (g + 1) * steps)

            @pl.when(g == 1)
            def _():
                for c in every_kv:
                    self.kv_copy(p, 0, c).wait_recv()
                self.attend(p, 1, 0, self.heads // HEADS_PER_STEP)

            for c in every_u:
                self.u_copy(p, g, c).wait_recv()
            norm_rows_into(self.t, self.uc.at[p], g * self.half, self.half, g1, b1)
            self.project_kv(p, g)
            return carry

        lax.fori_loop(0, 2, gather, 0)
        self.refill(0, i, count)
        filler()
        for c in every_kv:
            self.kv_copy(p, 1, c).wait_recv()
        self.attend(p, 2, 0, self.heads // HEADS_PER_STEP)
        for g in (None, 0, 1):
            for c in every_kv:
                self.kv_copy(p, g, c).wait_send()
        for idx in (1, 2, 3):
            self.weight(idx, i).wait()
        before_out()

        def finish(g, carry):
            at = self.group(g)
            self.t[at, :] = self.o[at, :].astype(BF)
            for lo, hi in col_tiles(self.width, 512):
                attn = mat_f32(self.t[at, :], self.wo[:, lo:hi])
                self.u2[at, lo:hi] = (self.u[at, lo:hi].astype(F32) + attn).astype(BF)
            norm_rows_into(self.t, self.u2, g * self.half, self.half, g2, b2)
            for lo, hi in col_tiles(self.hid.shape[1], 768):
                x = mat_f32(self.t[at, :], self.w1[:, lo:hi])
                gl = 0.5 * x * (1.0 + jnp.tanh(GELU_C * (x + 0.044715 * (x * x * x))))
                self.hid[:, lo:hi] = gl.astype(BF)
            for c in every_u:
                self.u_copy(0, g, c).wait_send()
            for c, (lo, hi) in enumerate(self.u_tiles):
                mlp = mat_f32(self.hid[...], self.w2[:, lo:hi])
                put(g, c, (self.u2[at, lo:hi].astype(F32) + mlp).astype(BF))
            return carry

        lax.fori_loop(0, 2, finish, 0)
        for idx in (1, 2, 3):
            self.refill(idx, i, count)


def barrier(me, flips):
    sem = pltpu.get_barrier_semaphore()
    for flip in flips:
        pl.semaphore_signal(sem, inc=1, device_id={"group": flipped(me, flip)}, device_id_type=MESH)
    pl.semaphore_wait(sem, len(flips))


COMMON = ("u", "u2", "uc", "t", "q", "kv", "o", "m", "l", "hid", "wqkv", "wo", "w1", "w2", "w_sem", "u_send", "u_recv", "kv_send", "kv_recv")


def common_scratch(rows, width, hidden, heads):
    u_n = len(col_tiles(width, U_TILE))
    kv_n = len(col_tiles(2 * width, KV_TILE))
    return [
        pltpu.VMEM((rows, width), BF),
        pltpu.VMEM((rows, width), BF),
        pltpu.VMEM((2, rows, width), BF),
        pltpu.VMEM((rows, width), BF),
        pltpu.VMEM((rows, width), BF),
        pltpu.VMEM((2, 4, rows, 2 * width), BF),
        pltpu.VMEM((rows, width), F32),
        pltpu.VMEM((heads, rows, 128), F32),
        pltpu.VMEM((heads, rows, 128), F32),
        pltpu.VMEM((rows // 2, hidden), BF),
        pltpu.VMEM((width, 3 * width), BF),
        pltpu.VMEM((width, width), BF),
        pltpu.VMEM((width, hidden), BF),
        pltpu.VMEM((hidden, width), BF),
        pltpu.SemaphoreType.DMA((6,)),
        pltpu.SemaphoreType.DMA((2, u_n)),
        pltpu.SemaphoreType.DMA((2, 2, u_n)),
        pltpu.SemaphoreType.DMA((3, kv_n)),
        pltpu.SemaphoreType.DMA((2, 3, kv_n)),
    ]


def in_kernel(heads, count, x_own, h_own, norms, hp_h, qkv_h, wo_h, w1_h, w2_h, wz_h, a_all, r_all, *scratch):
    refs = dict(zip(COMMON, scratch[:len(COMMON)]))
    wz, rbuf, r_send, r_recv, a_sem, x_sem = scratch[len(COMMON):]
    me = lax.axis_index("group")
    branch = lax.div(me, 4)
    blk = Block(me, refs, heads)
    blk.norm_of = lambda i: norms[branch, i].astype(F32)
    blk.w_src = [lambda i: qkv_h.at[branch, i], lambda i: wo_h.at[branch, i], lambda i: w1_h.at[branch, i],
                 lambda i: w2_h.at[branch, i], lambda i: wz_h.at[i]]
    blk.w_dst = [blk.wqkv, blk.wo, blk.w1, blk.w2, wz]
    hint_w = pltpu.make_async_copy(hp_h, wz, blk.w_sem.at[5])
    hint_w.start()
    for idx in range(4):
        blk.weight(idx, 0).start()
    barrier(me, (1, 2, 4))
    own = x_own.shape[0]

    give = blk.remote(blk.u2.at[0:own, :], blk.u.at[pl.ds(pl.multiple_of(branch * own, own), own), :],
                      x_sem.at[0], x_sem.at[1], 4)
    hint_w.wait()
    mine = pl.ds(pl.multiple_of(branch * own, own), own)
    for lo, hi in col_tiles(blk.width, 512):
        x = x_own[:, lo:hi]
        ctrl = (x.astype(F32) + mat_f32(h_own[...], wz[:, lo:hi])).astype(BF)
        blk.t[0:own, lo:hi] = ctrl

    @pl.when(branch == 0)
    def _():
        blk.u2[0:own, :] = blk.t[0:own, :]
        blk.u[mine, :] = x_own[...]

    @pl.when(branch == 1)
    def _():
        blk.u2[0:own, :] = x_own[...]
        blk.u[mine, :] = blk.t[0:own, :]
        blk.weight(4, 0).start()

    give.start()
    give.wait()
    for g in range(2):
        for c in range(len(blk.u_tiles)):
            blk.u_copy(0, g, c).start()

    def a_store(i):
        return pltpu.make_async_copy(blk.u, a_all.at[i], a_sem)

    def r_copy(j):
        par = lax.rem(j, 2)
        return pltpu.make_async_remote_copy(
            src_ref=rbuf.at[par], dst_ref=r_all.at[j], send_sem=r_send.at[par], recv_sem=r_recv.at[j],
            device_id={"group": lax.rem(me, 4)}, device_id_type=MESH)

    def make_r(j):
        @pl.when(j >= 2)
        def _():
            r_copy(j - 2).wait_send()

        blk.weight(4, j).wait()
        par = lax.rem(j, 2)
        for lo, hi in col_tiles(blk.width, 512):
            rbuf[par, :, lo:hi] = mat_f32(blk.u[...], wz[:, lo:hi]).astype(BF)
        r_copy(j).start()
        blk.refill(4, j, count)

    def layer(i, carry):
        def filler():
            @pl.when(jnp.logical_and(branch == 1, i >= 1))
            def _():
                make_r(i - 1)

        def before_out():
            @pl.when(i >= 1)
            def _():
                a_store(i - 1).wait()

        def put(g, c, values):
            lo, hi = blk.u_tiles[c]
            blk.u[blk.group(g), lo:hi] = values

            @pl.when(i + 1 < count)
            def _():
                blk.u_copy(1 - lax.rem(i, 2), g, c).start()

        blk.run(i, count, filler, before_out, put)
        a_store(i).start()
        return carry

    lax.fori_loop(0, count, layer, 0)

    @pl.when(branch == 1)
    def _():
        make_r(jnp.int32(count - 1))
        if count >= 2:
            r_copy(jnp.int32(count - 2)).wait_send()
        r_copy(jnp.int32(count - 1)).wait_send()

    @pl.when(branch == 0)
    def _():
        def take(j, carry):
            r_copy(j).wait_recv()
            return carry
        lax.fori_loop(0, count, take, 0)

    a_store(count - 1).wait()


def out_kernel(heads, count, a_all, r_all, norms, fin, qkv_h, wo_h, w1_h, w2_h, ws_h, wf_h, y, *scratch):
    refs = dict(zip(COMMON, scratch[:len(COMMON)]))
    top, low_w, low, o16, sa, sr, s_sem, y_sem = scratch[len(COMMON):]
    me = lax.axis_index("group")
    branch = lax.div(me, 4)
    own = y.shape[0]
    blk = Block(me, refs, heads)
    width = blk.width
    give = blk.remote(blk.u2.at[own:2 * own, :], y, y_sem.at[0], y_sem.at[1], 4)
    blk.norm_of = lambda i: norms[i].astype(F32)
    blk.w_src = [lambda i: qkv_h.at[i], lambda i: wo_h.at[i], lambda i: w1_h.at[i], lambda i: w2_h.at[i],
                 lambda i: ws_h.at[i, 0:width, :], lambda i: ws_h.at[i, width:2 * width, :]]
    blk.w_dst = [blk.wqkv, blk.wo, blk.w1, blk.w2, top, low_w]
    last_w = pltpu.make_async_copy(wf_h, blk.wo, blk.w_sem.at[1])

    def skip_load(j):
        idx = count - j
        return (pltpu.make_async_copy(a_all.at[idx], sa, s_sem.at[0]),
                pltpu.make_async_copy(r_all.at[idx], sr, s_sem.at[1]))

    def skip_sum(dst):
        for r in range(0, blk.rows, 32):
            dst[r:r + 32, :] = (sa[r:r + 32, :].astype(F32) + sr[r:r + 32, :].astype(F32)).astype(BF)

    def make_low(j):
        for cp in skip_load(j + 1):
            cp.wait()
        skip_sum(blk.t)

        @pl.when(j + 1 < count)
        def _():
            for cp in skip_load(j + 2):
                cp.start()

        blk.weight(5, j).wait()
        for lo, hi in col_tiles(width, 512):
            low[:, lo:hi] = mat_f32(blk.t[...], low_w[:, lo:hi])
        blk.refill(5, j, count)

    def merge(g, slot):
        at = blk.group(g)
        for c, (lo, hi) in enumerate(blk.u_tiles):
            blk.u[at, lo:hi] = (low[at, lo:hi] + mat_f32(o16[at, :], top[:, lo:hi])).astype(BF)
            blk.u_copy(slot, g, c).start()

    def run_all():
        for idx in (5, 4, 0, 1, 2, 3):
            blk.weight(idx, 0).start()
        for cp in skip_load(0):
            cp.start()
        barrier(me, (1, 2, 4))
        for cp in skip_load(0):
            cp.wait()
        skip_sum(o16)
        for cp in skip_load(1):
            cp.start()
        make_low(0)
        blk.weight(4, 0).wait()
        lax.fori_loop(0, 2, lambda g, carry: merge(g, 0) or carry, 0)
        blk.refill(4, 0, count)

        def layer(i, carry):
            def filler():
                @pl.when(i + 1 < count)
                def _():
                    make_low(i + 1)

            def before_out():
                @pl.when(i + 1 < count)
                def _():
                    blk.weight(4, i + 1).wait()

            def put(g, c, values):
                lo, hi = blk.u_tiles[c]
                o16[blk.group(g), lo:hi] = values
                if c == len(blk.u_tiles) - 1:
                    @pl.when(i + 1 < count)
                    def _():
                        merge(g, 1 - lax.rem(i, 2))

            blk.run(i, count, filler, before_out, put)
            blk.refill(4, i + 1, count)
            return carry

        lax.fori_loop(0, count, layer, 0)
        last_w.start()
        norm_rows_into(blk.t, o16, 0, blk.rows, fin[0:1, :].astype(F32), fin[1:2, :].astype(F32))
        last_w.wait()
        for r0, r1 in ((own, 2 * own), (0, own)):
            for lo, hi in col_tiles(width, 512):
                blk.u2[r0:r1, lo:hi] = mat_f32(blk.t[r0:r1, :], blk.wo[:, lo:hi]).astype(BF)
            if r0 > 0:
                give.start()
        y[...] = blk.u2[0:own, :]
        give.wait_send()

    pl.when(branch == 0)(run_all)

    @pl.when(branch == 1)
    def _():
        barrier(me, (4,))
        give.wait_recv()


def any_spec():
    return pl.BlockSpec(memory_space=pl.ANY)


def vmem_spec():
    return pl.BlockSpec(memory_space=pltpu.VMEM)


def solution(mesh):
    def device_step(x_own, hint_own, in_qkv, in_proj, in_up, in_down, in_norm, out_qkv, out_proj, out_up, out_down, out_norm, zero_proj, hint_proj, skip_proj, final_norm, w_out):
        n_in, n_out = zero_proj.shape[0], skip_proj.shape[0]
        tok_own, width = x_own.shape
        rows = 2 * tok_own
        hidden = in_up.shape[-1]
        heads = in_proj.shape[2]
        params = dict(vmem_limit_bytes=67_000_000, has_side_effects=True)
        a_all, r_all = pl.pallas_call(
            functools.partial(in_kernel, heads, n_in),
            name="in_phase",
            out_shape=[jax.ShapeDtypeStruct((n_in, rows, width), BF)] * 2,
            in_specs=[vmem_spec()] * 3 + [any_spec()] * 6,
            out_specs=[any_spec(), any_spec()],
            scratch_shapes=common_scratch(rows, width, hidden, heads) + [
                pltpu.VMEM((width, width), BF),
                pltpu.VMEM((2, rows, width), BF),
                pltpu.SemaphoreType.DMA((2,)),
                pltpu.SemaphoreType.DMA((n_in,)),
                pltpu.SemaphoreType.DMA,
                pltpu.SemaphoreType.DMA((2,)),
            ],
            compiler_params=pltpu.CompilerParams(collective_id=0, **params),
        )(x_own, hint_own, in_norm, hint_proj, in_qkv, in_proj.reshape(2, n_in, width, width), in_up, in_down, zero_proj)
        return pl.pallas_call(
            functools.partial(out_kernel, heads, n_out),
            name="out_phase",
            out_shape=jax.ShapeDtypeStruct((tok_own, width), BF),
            in_specs=[any_spec()] * 2 + [vmem_spec()] * 2 + [any_spec()] * 6,
            out_specs=vmem_spec(),
            scratch_shapes=common_scratch(rows, width, hidden, heads) + [
                pltpu.VMEM((width, width), BF),
                pltpu.VMEM((width, width), BF),
                pltpu.VMEM((rows, width), F32),
                pltpu.VMEM((rows, width), BF),
                pltpu.VMEM((rows, width), BF),
                pltpu.VMEM((rows, width), BF),
                pltpu.SemaphoreType.DMA((2,)),
                pltpu.SemaphoreType.DMA((2,)),
            ],
            compiler_params=pltpu.CompilerParams(collective_id=1, **params),
        )(a_all, r_all, out_norm, final_norm, out_qkv, out_proj.reshape(n_out, width, width), out_up, out_down, skip_proj, w_out)

    tok_spec = P(("data", "group"), None)
    return jax.shard_map(device_step, mesh=mesh, in_specs=(tok_spec, tok_spec) + (P(),) * 15, out_specs=tok_spec, check_vma=False)
```
